32 devices in a mesh: gx: 4 (over z), gy: 4 (over x, core), gz: 2 (over y).
Axes of the slice: x: 2, y: 2, z: 4, core: 2. Of those that a mesh axis runs over, the one named last changes fastest.
Arguments:
- state: float32 [7, 64, 64, 256], P(None, 'gx', 'gy', 'gz'), may hold values from -1 to 4, as said below
- solver_owner: int32 [4, 2, 8], P('gy', 'gz'), may hold values from 0 to 15, as said below
- phi_prev: float32 [16, 8, 64, 256], P('gx', None, 'gy', 'gz'), may hold values from -1.2 to 1.2
Outputs:
- new_state: float32 [7, 64, 64, 256], P(None, 'gx', 'gy', 'gz')
- density_solver: float32 [16, 8, 64, 256], P('gx', None, 'gy', 'gz')
- residual: float32 [64, 64, 256], P('gx', 'gy', 'gz')
The draws below stay inside these ranges and needn't reach their ends.
Inputs may be any that keep to these rules, and one draw needn't show every extreme that they name: `state`: field 0 lies in [1, 2], fields 1 to 3 in [-1, 1], field 4 in [2, 4], field 5 in [1, 2], field 6 in [0, 1]. `solver_owner`: entry b of line (j, k) is owner * 4 + slot, the owner being the gx index holding box b in the solver ownership. Codes within a line are distinct, so an owner holds at most 4 boxes of a line, and in every line some owner holds exactly 4.
All inputs are finite; a program needn't handle non-finite values.
Results may differ from the reference program's by a relative error of at most 0.00012.
Values sent between devices are 32-bit elements; how exact they have to be, the bound alone decides.
A program may use at most 64 MiB of HBM per device.

```python
import jax
import jax.numpy as jnp
from jax import lax

CY = 16
CZ = 128
SLOTS = 4
BX = 8
LINES_Y = 4
LINES_Z = 2
BOXES = 8
CODES = 16
NX = 64
NY = 64
NZ = 256


def draw_state(key, part):
    keys = jax.random.split(key, 6)
    shape = (NX, NY, NZ)
    density = jnp.exp(jax.random.uniform(keys[0], shape, jnp.float32) * jnp.log(2.0))
    momenta = jnp.clip(0.4 * jax.random.normal(keys[2], (3,) + shape, jnp.float32), -1.0, 1.0)
    energy = jax.random.uniform(keys[3], shape, jnp.float32, 2.0, 4.0)
    internal = jax.random.uniform(keys[4], shape, jnp.float32, 1.0, 2.0)
    tracer = jax.random.uniform(keys[5], shape, jnp.float32)
    stacked = jnp.concatenate([density[None], momenta, energy[None], internal[None], tracer[None]], 0)
    return stacked.astype(jnp.float32)


def owner_line(key):
    keys = jax.random.split(key, 3)
    fullest = jax.random.randint(keys[0], (), 0, CODES // SLOTS)
    index = jnp.arange(CODES, dtype=jnp.int32)
    scores = jax.random.randint(keys[1], (CODES,), 0, 1 << 20) * CODES + index
    scores = jnp.where(index // SLOTS == fullest, index - CODES, scores)
    order = jnp.argsort(scores, stable=True).astype(jnp.int32)
    chosen = order[:BOXES]
    placing = jax.random.permutation(keys[2], BOXES)
    return jnp.zeros((BOXES,), jnp.int32).at[placing].set(chosen)


def draw_solver_owner(key, part):
    keys = jax.random.split(key, LINES_Y * LINES_Z)
    lines = jax.vmap(owner_line)(keys)
    return lines.reshape(LINES_Y, LINES_Z, BOXES).astype(jnp.int32)


def levels(rng, extent, pieces, low, largest):
    def one(axis_at, shards_of):
        draws = jax.random.uniform(jax.random.fold_in(jax.random.fold_in(rng, 6), axis_at), (shards_of,), jnp.float32, low / len(pieces), largest / len(pieces))
        return jnp.repeat(jnp.exp(draws), extent[axis_at] // shards_of).reshape((-1,) + (1,) * (len(extent) - axis_at - 1))

    loudness = one(*pieces[0])
    for cut in pieces[1:]:
        loudness = loudness * one(*cut)
    return loudness


def scatter_about(own_key, shape, scale, reach, cuts=(), kind=jnp.bfloat16):
    loudness = levels(own_key, shape, cuts, -0.22, 0.18) if cuts else 1.0
    entries = jax.random.normal(own_key, shape, jnp.float32) * scale * loudness
    return jnp.minimum(jnp.maximum(entries, -reach), reach).astype(kind)


def setup_inputs(seed: int = 0) -> dict:
    key_list = jax.random.split(jax.random.key(seed), 4)
    state = draw_state(jax.random.fold_in(key_list[3], 71), 0)
    solver_owner = draw_solver_owner(jax.random.fold_in(key_list[3], 71), 0)
    phi_prev = scatter_about(key_list[2], (CODES, BX, NY, NZ), 0.2, 1.2, ((0, 4), (2, 4), (3, 2)), jnp.float32)
    return {"state": state, "solver_owner": solver_owner, "phi_prev": phi_prev}


GAMMA = 5.0 / 3.0
DTH = 0.04
FOURPIG = 2.0

def wave_speed(q, d):
    dens = jnp.maximum(q[0], 0.25)
    vel = q[d] / dens
    press = (GAMMA - 1.0) * jnp.maximum(q[5], 0.1)
    return jnp.abs(vel) + jnp.sqrt(GAMMA * press / dens)

def physical_flux(v, d):
    dens = jnp.maximum(v[0], 0.25)
    vel = v[d] / dens
    press = (GAMMA - 1.0) * jnp.maximum(v[5], 0.1)
    comps = [v[d]]
    for k in (1, 2, 3):
        term = v[k] * vel
        if k == d:
            term = term + press
        comps.append(term)
    comps.append((v[4] + press) * vel)
    comps.append(v[5] * vel)
    comps.append(v[6] * vel)
    return jnp.stack(comps, 0)

def tendency(padded):
    total = None
    for d in (1, 2, 3):
        line = padded
        for e in (1, 2, 3):
            if e != d:
                line = lax.slice_in_dim(line, 2, line.shape[e] - 2, axis=e)
        count = line.shape[d] - 3
        left_far = lax.slice_in_dim(line, 0, count, axis=d)
        left = lax.slice_in_dim(line, 1, count + 1, axis=d)
        right = lax.slice_in_dim(line, 2, count + 2, axis=d)
        right_far = lax.slice_in_dim(line, 3, count + 3, axis=d)
        edge = 7.0 / 12.0 * (left + right) - 1.0 / 12.0 * (left_far + right_far)
        edge = jnp.clip(edge, jnp.minimum(left, right), jnp.maximum(left, right))
        speed = wave_speed(line, d)
        fastest = jnp.maximum(lax.slice_in_dim(speed, 1, count + 1, axis=d - 1), lax.slice_in_dim(speed, 2, count + 2, axis=d - 1))
        flux = physical_flux(edge, d) - 0.5 * fastest[None] * (right - left)
        change = lax.slice_in_dim(flux, 1, count, axis=d) - lax.slice_in_dim(flux, 0, count - 1, axis=d)
        total = change if total is None else total + change
    return -total

def wrapped(q):
    return jnp.pad(q, ((0, 0), (2, 2), (2, 2), (2, 2)), mode='wrap')

def reference(state, solver_owner, phi_prev):
    first = state + DTH * tendency(wrapped(state))
    new_state = 0.5 * state + 0.5 * (first + DTH * tendency(wrapped(first)))
    density = new_state[0]
    onehot = (solver_owner[..., None] == jnp.arange(CODES, dtype=jnp.int32)).astype(jnp.float32)
    boxes = density.reshape(BOXES, BX, LINES_Y, CY, LINES_Z, CZ).astype(jnp.float32)
    density_solver = jnp.einsum('jkbc,bxjykz->cxjykz', onehot, boxes, precision=lax.Precision.HIGHEST).reshape(CODES, BX, NY, NZ)
    slots_phi = phi_prev.reshape(CODES, BX, LINES_Y, CY, LINES_Z, CZ).astype(jnp.float32)
    potential = jnp.einsum('jkbc,cxjykz->bxjykz', onehot, slots_phi, precision=lax.Precision.HIGHEST).reshape(NX, NY, NZ)
    beside_all = jnp.zeros_like(potential)
    for axis in (0, 1, 2):
        beside_all = beside_all + jnp.roll(potential, 1, axis) + jnp.roll(potential, -1, axis)
    laplace = beside_all - 6.0 * potential
    mean = jnp.sum(density) / (NX * NY * NZ)
    residual = FOURPIG * (density - mean) - laplace
    return (new_state, density_solver, residual)
```

```python
import functools

import jax
import jax.numpy as jnp
from jax import lax
from jax.experimental import pallas as pl
from jax.experimental.pallas import tpu as pltpu
from jax.sharding import PartitionSpec as P

GAMMA = 5.0 / 3.0
DTH = 0.04
FOURPIG = 2.0
PAD = 8
AXES = ("gx", "gy", "gz")


def edge_value(a, b, c, d):
    e = 7.0 / 12.0 * (b + c) - 1.0 / 12.0 * (a + d)
    return jnp.minimum(jnp.maximum(e, jnp.minimum(b, c)), jnp.maximum(b, c))


def sound(q0, q5):
    rinv = 1.0 / jnp.maximum(q0, 0.25)
    return rinv, jnp.sqrt((GAMMA * (GAMMA - 1.0)) * jnp.maximum(q5, 0.1) * rinv)


def speed_of(q, d):
    rinv, c = sound(q[0], q[5])
    return jnp.abs(q[d]) * rinv + c


def interface_flux(a, b, c, d, far, direction):
    n = len(b)
    e = [edge_value(a[f], b[f], c[f], d[f]) for f in range(n)]
    vel = e[direction] / jnp.maximum(e[0], 0.25)
    press = (GAMMA - 1.0) * jnp.maximum(e[5], 0.1)
    half = 0.5 * far
    out = [e[direction]]
    for k in (1, 2, 3):
        term = e[k] * vel
        out.append(term + press if k == direction else term)
    out.append((e[4] + press) * vel)
    for k in range(5, n):
        out.append(e[k] * vel)
    return [out[f] - half * (c[f] - b[f]) for f in range(n)]


def lanes_change(q, s):
    n = q[0].shape[1]
    low = [pltpu.roll(v, 1, 1) for v in q]
    high = [pltpu.roll(v, n - 1, 1) for v in q]
    higher = [pltpu.roll(v, n - 2, 1) for v in q]
    flux = interface_flux(low, q, high, higher, jnp.maximum(s, pltpu.roll(s, n - 1, 1)), 3)
    return [v - pltpu.roll(v, 1, 1) for v in flux]


def kernel(
    shape, codes, state, phi, new_state, density_solver, residual,
    Q1, Q2, Qp, Sy1, Sy2, Syp, Ry1, Ry2, Ryp, Pz, Pzp, Rz, Rzp_, T, RC, FL, SN, C, Cp,
    PH, Ps, Pr, NS, Dg, DS, RS, M, Mx, My, Mz, send_sem, recv_sem, local_sem,
):
    sizes, fields, cx, cy, cz, slots, half = shape
    gx, gy, gz = sizes
    me = [lax.axis_index(a) for a in AXES]
    peer = lambda i, k: {AXES[i]: lax.rem(me[i] + k, sizes[i])}
    used = [0]
    sends = []

    def send(src, dst, to):
        i = used[0]
        used[0] += 1
        copy = pltpu.make_async_remote_copy(
            src_ref=src, dst_ref=dst, send_sem=send_sem.at[i], recv_sem=recv_sem.at[i],
            device_id=to, device_id_type=pl.DeviceIdType.MESH,
        )
        copy.start()
        sends.append(copy)
        return copy

    load_state = pltpu.make_async_copy(
        state, Q1.at[:, pl.ds(2, cx), pl.ds(PAD, cy)], local_sem.at[0]
    )
    load_state.start()
    load_phi = pltpu.make_async_copy(phi, PH, local_sem.at[1])
    load_phi.start()

    barrier = pltpu.get_barrier_semaphore()
    for i in range(3):
        for k in range(1, sizes[i]):
            pl.semaphore_signal(
                barrier, inc=1, device_id=peer(i, k), device_id_type=pl.DeviceIdType.MESH
            )

    lane = lax.broadcasted_iota(jnp.int32, (cy, cz), 1)
    row = lax.broadcasted_iota(jnp.int32, (cy, cz), 0)
    group = lane // 8
    low_half = lane % 8 < 4
    inner = slice(PAD, PAD + cy)

    def pack_y(Q, Sy, n):
        flat = Q.reshape(n * (cx + 4) * (cy + 2 * PAD), cz)
        for f in range(n):
            for r, y in enumerate((0, 1, cy - 2, cy - 1)):
                at = (f * (cx + 4) + 2) * (cy + 2 * PAD) + PAD + y
                Sy[f, r] = flat[pl.ds(at, cx, stride=cy + 2 * PAD), :]

    def unpack_y(Q, Ry, n):
        flat = Q.reshape(n * (cx + 4) * (cy + 2 * PAD), cz)
        for f in range(n):
            for r, y in enumerate((-2, -1, cy, cy + 1)):
                at = (f * (cx + 4) + 2) * (cy + 2 * PAD) + PAD + y
                flat[pl.ds(at, cx, stride=cy + 2 * PAD), :] = Ry[f, r]

    def pack_z(Q, Pz, n):
        def step(x, packed):
            return tuple(
                jnp.where(group == x, pltpu.roll(Q[f, x + 2, inner, :], 4 + 8 * x, 1), packed[f])
                for f in range(n)
            )

        packed = lax.fori_loop(0, cx, step, tuple(jnp.zeros((cy, cz), jnp.float32) for _ in range(n)))
        for f in range(n):
            Pz[f] = packed[f]

    def exchange(Q, Sy, Ry, Pz, Rz):
        x = [
            send(Q.at[:, pl.ds(cx, 2), pl.ds(PAD, cy)], Q.at[:, pl.ds(0, 2), pl.ds(PAD, cy)], peer(0, 1)),
            send(Q.at[:, pl.ds(2, 2), pl.ds(PAD, cy)], Q.at[:, pl.ds(cx + 2, 2), pl.ds(PAD, cy)], peer(0, gx - 1)),
        ]
        y = [
            send(Sy.at[:, pl.ds(2, 2)], Ry.at[:, pl.ds(0, 2)], peer(1, 1)),
            send(Sy.at[:, pl.ds(0, 2)], Ry.at[:, pl.ds(2, 2)], peer(1, gy - 1)),
        ]
        z = [send(Pz, Rz.at[0], peer(2, 1))]
        if gz > 2:
            z.append(send(Pz, Rz.at[1], peer(2, gz - 1)))
        return x, y, z

    def from_both(Rz):
        return Rz.at[0], Rz.at[1 if gz > 2 else 0]

    def z_main(Q):
        def step(x, carry):
            q = [Q[f, x + 2, inner, :] for f in range(fields)]
            rinv, c = sound(q[0], q[5])
            RC[0, x] = rinv
            RC[1, x] = c
            change = lanes_change(q, jnp.abs(q[3]) * rinv + c)
            for f in range(fields):
                T[f, x] = change[f]
            return carry

        lax.fori_loop(0, cx, step, 0)

    def finish(Q, Sy, Ry, Pz, Rz, update):
        prev, nxt = from_both(Rz)
        left = [jnp.where(low_half, prev[f], Pz[f]) for f in range(fields)]
        left = lanes_change(left, speed_of(left, 3))
        right = [jnp.where(low_half, Pz[f], nxt[f]) for f in range(fields)]
        right = lanes_change(right, speed_of(right, 3))
        for f in range(fields):
            C[f] = jnp.where(low_half, right[f], left[f])
        unpack_y(Q, Ry, fields)
        b = [Ry[f, 1] for f in range(fields)]
        c = [Sy[f, 0] for f in range(fields)]
        flux = interface_flux(
            [Ry[f, 0] for f in range(fields)], b, c, [Sy[f, 1] for f in range(fields)],
            jnp.maximum(speed_of(b, 2), speed_of(c, 2)), 2,
        )
        for f in range(fields):
            FL[f] = flux[f]
        SN[...] = speed_of([Ry[f, 2] for f in range(fields)], 2)

        def x_flux(x, s):
            rows = [[Q[f, x + k, inner, :] for f in range(fields)] for k in range(1, 5)]
            s_next = speed_of(rows[2], 1)
            return interface_flux(*rows, jnp.maximum(s, s_next), 1), s_next

        def step(x, carry):
            before, s = carry
            after, s_next = x_flux(x, s)
            cells = [[Q[f, x + 2, PAD + k : PAD + k + cy, :] for f in range(fields)] for k in (-1, 0, 1, 2)]
            sy = jnp.abs(cells[1][2]) * RC[0, x] + RC[1, x]
            sy_next = jnp.where(row == cy - 1, SN[pl.ds(x, 1), :], pltpu.roll(sy, cy - 1, 0))
            flux = interface_flux(*cells, jnp.maximum(sy, sy_next), 2)
            outer = (lane < 2) | (lane >= cz - 2)
            for f in range(fields):
                low = jnp.where(row == 0, FL[f, pl.ds(x, 1), :], pltpu.roll(flux[f], 1, 0))
                along_z = jnp.where(outer, pltpu.roll(C[f], cz - 4 - 8 * x, 1), T[f, x])
                total = (after[f] - before[f]) + (flux[f] - low) + along_z
                update(f, x, cells[1][f], total)
            return tuple(after), s_next

        s = speed_of([Q[f, 1, inner, :] for f in range(fields)], 1)
        start, s = x_flux(-1, s)
        lax.fori_loop(0, cx, step, (tuple(start), s))

    load_state.wait()
    pack_y(Q1, Sy1, fields)
    pack_z(Q1, Pz.at[0], fields)
    mass = lax.fori_loop(
        0, cx, lambda x, m: m + Q1[0, x + 2, inner, :], jnp.zeros((cy, cz), jnp.float32)
    )
    M[0] = mass[:8] + mass[8:] if cy == 16 else jnp.broadcast_to(jnp.sum(mass, 0, keepdims=True) / 8, (8, cz))
    pl.semaphore_wait(barrier, gx + gy + gz - 3)
    x1, y1, z1 = exchange(Q1, Sy1, Ry1, Pz.at[0], Rz.at[0])
    masses = [send(M.at[0], Mx.at[k - 1], peer(0, k)) for k in range(1, gx)]

    load_phi.wait()
    boxes = cx // half

    def owned(holder, j):
        slot = codes[0, 0, holder * boxes + j] - me[0] * slots
        mine = (slot >= 0) & (slot < slots)
        return jnp.where(mine, PH[jnp.clip(slot, 0, slots - 1)], 0.0)

    phis = []
    for k in range(1, gx):
        for j in range(boxes):
            Ps[k - 1, j] = owned(lax.rem(me[0] + k, gx), j)
        phis.append(send(Ps.at[k - 1], Pr.at[k - 1], peer(0, k)))

    z_main(Q1)

    for copy in masses:
        copy.wait_recv()
    M[1] = M[0] + sum(Mx[k] for k in range(gx - 1))
    masses = [send(M.at[1], My.at[k - 1], peer(1, k)) for k in range(1, gy)]

    for copy in x1 + y1 + z1:
        copy.wait_recv()

    def to_first(f, x, q, total):
        Q2[f, x + 2, inner, :] = q - DTH * total

    finish(Q1, Sy1, Ry1, Pz.at[0], Rz.at[0], to_first)
    pack_y(Q2, Sy2, fields)
    pack_z(Q2, Pz.at[1], fields)
    x2, y2, z2 = exchange(Q2, Sy2, Ry2, Pz.at[1], Rz.at[1])

    for copy in masses:
        copy.wait_recv()
    M[2] = M[1] + sum(My[k] for k in range(gy - 1))
    masses = [send(M.at[2], Mz.at[k - 1], peer(2, k)) for k in range(1, gz)]

    z_main(Q2)

    for copy in x2 + y2 + z2:
        copy.wait_recv()

    def to_new(f, x, q, total):
        value = 0.5 * Q1[f, x + 2, inner, :] + 0.5 * (q - DTH * total)
        NS[f, x] = value
        if f == 0:
            Dg[me[0] * boxes + x // half, x % half] = value

    finish(Q2, Sy2, Ry2, Pz.at[1], Rz.at[1], to_new)
    mine = Dg.at[pl.ds(me[0] * boxes, boxes)]
    dens = [send(mine, mine, peer(0, k)) for k in range(1, gx)]
    out_state = pltpu.make_async_copy(NS, new_state, local_sem.at[2])
    out_state.start()

    for copy in phis:
        copy.wait_recv()
    for j in range(boxes):
        box = owned(me[0], j)
        for k in range(gx - 1):
            box = box + Pr[k, j]
        Qp[0, 2 + j * half : 2 + (j + 1) * half, inner, :] = box
    pack_y(Qp, Syp, 1)
    pack_z(Qp, Pzp, 1)
    xp, yp, zp = exchange(Qp, Syp, Ryp, Pzp, Rzp_)
    for copy in masses:
        copy.wait_recv()
    total = M[2] + sum(Mz[k] for k in range(gz - 1))
    mean = jnp.sum(total) * (1.0 / (cx * cy * cz * gx * gy * gz))
    for copy in xp + yp + zp:
        copy.wait_recv()
    unpack_y(Qp, Ryp, 1)
    prev, nxt = from_both(Rzp_)
    beside = lambda v: pltpu.roll(v, 1, 1) + pltpu.roll(v, cz - 1, 1)
    Cp[...] = jnp.where(
        low_half, beside(jnp.where(low_half, Pzp[0], nxt[0])), beside(jnp.where(low_half, prev[0], Pzp[0]))
    )

    def poisson(x, carry):
        q = Qp[0, x + 2, inner, :]
        along_z = jnp.where((lane == 0) | (lane == cz - 1), pltpu.roll(Cp[...], cz - 4 - 8 * x, 1), beside(q))
        near = Qp[0, x + 1, inner, :] + Qp[0, x + 3, inner, :]
        near = near + Qp[0, x + 2, PAD - 1 : PAD - 1 + cy, :] + Qp[0, x + 2, PAD + 1 : PAD + 1 + cy, :]
        RS[x] = FOURPIG * (NS[0, x] - mean) - (near + along_z - 6.0 * q)
        return carry

    lax.fori_loop(0, cx, poisson, 0)
    out_residual = pltpu.make_async_copy(RS, residual, local_sem.at[3])
    out_residual.start()

    for copy in dens:
        copy.wait_recv()
    for s in range(slots):
        wanted = me[0] * slots + s
        at = jnp.int32(-1)
        for b in range(gx * boxes):
            at = jnp.where(codes[0, 0, b] == wanted, b, at)
        DS[s] = jnp.where(at >= 0, Dg[jnp.maximum(at, 0)], 0.0)
    out_density = pltpu.make_async_copy(DS, density_solver, local_sem.at[4])
    out_density.start()
    for copy in sends:
        copy.wait_send()
    out_state.wait()
    out_residual.wait()
    out_density.wait()


def on_device(sizes, state, solver_owner, phi_prev):
    fields, cx, cy, cz = state.shape
    slots, half = phi_prev.shape[:2]
    gx, gy, gz = sizes
    boxes = cx // half
    f32 = lambda *s: pltpu.VMEM(s, jnp.float32)
    padded = (cx + 4, cy + 2 * PAD, cz)
    n_send = 3 * (4 + min(gz - 1, 2)) + 3 * (gx - 1) + (gy - 1) + (gz - 1)
    out = lambda *s: jax.ShapeDtypeStruct(s, jnp.float32)
    hbm = pl.BlockSpec(memory_space=pl.ANY)
    return pl.pallas_call(
        functools.partial(kernel, (sizes, fields, cx, cy, cz, slots, half)),
        out_shape=(out(*state.shape), out(*phi_prev.shape), out(cx, cy, cz)),
        in_specs=[pl.BlockSpec(memory_space=pltpu.SMEM), hbm, hbm],
        out_specs=(hbm, hbm, hbm),
        scratch_shapes=[
            f32(fields, *padded), f32(fields, *padded), f32(1, *padded),
            f32(fields, 4, cx, cz), f32(fields, 4, cx, cz), f32(1, 4, cx, cz),
            f32(fields, 4, cx, cz), f32(fields, 4, cx, cz), f32(1, 4, cx, cz),
            f32(2, fields, cy, cz), f32(1, cy, cz), f32(2, 2, fields, cy, cz), f32(2, 1, cy, cz),
            f32(fields, cx, cy, cz), f32(2, cx, cy, cz), f32(fields, cx, cz), f32(cx, cz),
            f32(fields, cy, cz), f32(cy, cz),
            f32(slots, half, cy, cz), f32(gx - 1, boxes, half, cy, cz), f32(gx - 1, boxes, half, cy, cz),
            f32(fields, cx, cy, cz), f32(gx * boxes, half, cy, cz), f32(slots, half, cy, cz), f32(cx, cy, cz),
            f32(3, 8, cz), f32(gx - 1, 8, cz), f32(gy - 1, 8, cz), f32(gz - 1, 8, cz),
            pltpu.SemaphoreType.DMA((n_send,)), pltpu.SemaphoreType.DMA((n_send,)), pltpu.SemaphoreType.DMA((5,)),
        ],
        compiler_params=pltpu.CompilerParams(
            collective_id=0, has_side_effects=True, vmem_limit_bytes=63 * 1024 * 1024
        ),
    )(solver_owner, state, phi_prev)


def solution(mesh):
    sizes = tuple(mesh.shape[a] for a in AXES)
    placed = (P(None, "gx", "gy", "gz"), P("gy", "gz", None), P("gx", None, "gy", "gz"))
    return jax.shard_map(
        functools.partial(on_device, sizes),
        mesh=mesh,
        in_specs=placed,
        out_specs=(P(None, "gx", "gy", "gz"), P("gx", None, "gy", "gz"), P("gx", "gy", "gz")),
        check_vma=False,
    )
```

```python
import functools

import jax
import jax.numpy as jnp
from jax import lax
from jax.experimental import pallas as pl
from jax.experimental.pallas import tpu as pltpu
from jax.sharding import PartitionSpec as P

GAMMA = 5.0 / 3.0
DTH = 0.04
FOURPIG = 2.0
PAD = 8
AXES = ("gx", "gy", "gz")


def edge_value(a, b, c, d):
    e = 7.0 / 12.0 * (b + c) - 1.0 / 12.0 * (a + d)
    return jnp.minimum(jnp.maximum(e, jnp.minimum(b, c)), jnp.maximum(b, c))


def sound(q0, q5):
    rinv = 1.0 / jnp.maximum(q0, 0.25)
    return rinv, jnp.sqrt((GAMMA * (GAMMA - 1.0)) * jnp.maximum(q5, 0.1) * rinv)


def speed_of(q, d):
    rinv, c = sound(q[0], q[5])
    return jnp.abs(q[d]) * rinv + c


def interface_flux(a, b, c, d, far, direction):
    n = len(b)
    e = [edge_value(a[f], b[f], c[f], d[f]) for f in range(n)]
    vel = e[direction] / jnp.maximum(e[0], 0.25)
    press = (GAMMA - 1.0) * jnp.maximum(e[5], 0.1)
    half = 0.5 * far
    out = [e[direction]]
    for k in (1, 2, 3):
        term = e[k] * vel
        out.append(term + press if k == direction else term)
    out.append((e[4] + press) * vel)
    for k in range(5, n):
        out.append(e[k] * vel)
    return [out[f] - half * (c[f] - b[f]) for f in range(n)]


def lanes_change(q, s):
    n = q[0].shape[1]
    low = [pltpu.roll(v, 1, 1) for v in q]
    high = [pltpu.roll(v, n - 1, 1) for v in q]
    higher = [pltpu.roll(v, n - 2, 1) for v in q]
    flux = interface_flux(low, q, high, higher, jnp.maximum(s, pltpu.roll(s, n - 1, 1)), 3)
    return [v - pltpu.roll(v, 1, 1) for v in flux]


def kernel(
    shape, codes, state, phi, new_state, density_solver, residual,
    Q1, Q2, Qp, Sy1, Sy2, Syp, Ry1, Ry2, Ryp, Pz, Pzp, Rz, Rzp_, T, RC, FL, SN, C, Cp,
    PH, Ps, Pr, Pf, NS, Dg, DS, RS, M, Mx, My, Mz, send_sem, recv_sem, local_sem,
):
    sizes, fields, cx, cy, cz, slots, half = shape
    gx, gy, gz = sizes
    me = [lax.axis_index(a) for a in AXES]
    peer = lambda i, k: {AXES[i]: lax.rem(me[i] + k, sizes[i])}
    used = [0]
    sends = []

    def send(src, dst, to):
        i = used[0]
        used[0] += 1
        copy = pltpu.make_async_remote_copy(
            src_ref=src, dst_ref=dst, send_sem=send_sem.at[i], recv_sem=recv_sem.at[i],
            device_id=to, device_id_type=pl.DeviceIdType.MESH,
        )
        copy.start()
        sends.append(copy)
        return copy

    def channel():
        used[0] += 1
        return used[0] - 1

    def copy_on(i, src, dst, to):
        return pltpu.make_async_remote_copy(
            src_ref=src, dst_ref=dst, send_sem=send_sem.at[i], recv_sem=recv_sem.at[i],
            device_id=to, device_id_type=pl.DeviceIdType.MESH,
        )

    some_sends = []

    def send_if(i, cond, src, dst, to):
        pl.when(cond)(lambda: copy_on(i, src, dst, to).start())
        some_sends.append((cond, i, src))

    def wait_if(i, cond, dst):
        pl.when(cond)(lambda: copy_on(i, dst, dst, peer(0, 1)).wait_recv())

    load_state = pltpu.make_async_copy(
        state, Q1.at[:, pl.ds(2, cx), pl.ds(PAD, cy)], local_sem.at[0]
    )
    load_state.start()
    load_phi = pltpu.make_async_copy(phi, PH, local_sem.at[1])
    load_phi.start()

    barrier = pltpu.get_barrier_semaphore()
    for i in range(3):
        for k in range(1, sizes[i]):
            pl.semaphore_signal(
                barrier, inc=1, device_id=peer(i, k), device_id_type=pl.DeviceIdType.MESH
            )

    lane = lax.broadcasted_iota(jnp.int32, (cy, cz), 1)
    row = lax.broadcasted_iota(jnp.int32, (cy, cz), 0)
    group = lane // 8
    low_half = lane % 8 < 4
    inner = slice(PAD, PAD + cy)

    def pack_y(Q, Sy, n):
        flat = Q.reshape(n * (cx + 4) * (cy + 2 * PAD), cz)
        for f in range(n):
            for r, y in enumerate((0, 1, cy - 2, cy - 1)):
                at = (f * (cx + 4) + 2) * (cy + 2 * PAD) + PAD + y
                Sy[f, r] = flat[pl.ds(at, cx, stride=cy + 2 * PAD), :]

    def unpack_y(Q, Ry, n):
        flat = Q.reshape(n * (cx + 4) * (cy + 2 * PAD), cz)
        for f in range(n):
            for r, y in enumerate((-2, -1, cy, cy + 1)):
                at = (f * (cx + 4) + 2) * (cy + 2 * PAD) + PAD + y
                flat[pl.ds(at, cx, stride=cy + 2 * PAD), :] = Ry[f, r]

    def pack_z(Q, Pz, n):
        def step(x, packed):
            return tuple(
                jnp.where(group == x, pltpu.roll(Q[f, x + 2, inner, :], 4 + 8 * x, 1), packed[f])
                for f in range(n)
            )

        packed = lax.fori_loop(0, cx, step, tuple(jnp.zeros((cy, cz), jnp.float32) for _ in range(n)))
        for f in range(n):
            Pz[f] = packed[f]

    def exchange(Q, Sy, Ry, Pz, Rz):
        x = [
            send(Q.at[:, pl.ds(cx, 2), pl.ds(PAD, cy)], Q.at[:, pl.ds(0, 2), pl.ds(PAD, cy)], peer(0, 1)),
            send(Q.at[:, pl.ds(2, 2), pl.ds(PAD, cy)], Q.at[:, pl.ds(cx + 2, 2), pl.ds(PAD, cy)], peer(0, gx - 1)),
        ]
        y = [
            send(Sy.at[:, pl.ds(2, 2)], Ry.at[:, pl.ds(0, 2)], peer(1, 1)),
            send(Sy.at[:, pl.ds(0, 2)], Ry.at[:, pl.ds(2, 2)], peer(1, gy - 1)),
        ]
        z = [send(Pz, Rz.at[0], peer(2, 1))]
        if gz > 2:
            z.append(send(Pz, Rz.at[1], peer(2, gz - 1)))
        return x, y, z

    def from_both(Rz):
        return Rz.at[0], Rz.at[1 if gz > 2 else 0]

    def z_main(Q):
        def step(x, carry):
            q = [Q[f, x + 2, inner, :] for f in range(fields)]
            rinv, c = sound(q[0], q[5])
            RC[0, x] = rinv
            RC[1, x] = c
            change = lanes_change(q, jnp.abs(q[3]) * rinv + c)
            for f in range(fields):
                T[f, x] = change[f]
            return carry

        lax.fori_loop(0, cx, step, 0, unroll=2)

    def finish(Q, Sy, Ry, Pz, Rz, update):
        prev, nxt = from_both(Rz)
        left = [jnp.where(low_half, prev[f], Pz[f]) for f in range(fields)]
        left = lanes_change(left, speed_of(left, 3))
        right = [jnp.where(low_half, Pz[f], nxt[f]) for f in range(fields)]
        right = lanes_change(right, speed_of(right, 3))
        for f in range(fields):
            C[f] = jnp.where(low_half, right[f], left[f])
        unpack_y(Q, Ry, fields)
        b = [Ry[f, 1] for f in range(fields)]
        c = [Sy[f, 0] for f in range(fields)]
        flux = interface_flux(
            [Ry[f, 0] for f in range(fields)], b, c, [Sy[f, 1] for f in range(fields)],
            jnp.maximum(speed_of(b, 2), speed_of(c, 2)), 2,
        )
        for f in range(fields):
            FL[f] = flux[f]
        SN[...] = speed_of([Ry[f, 2] for f in range(fields)], 2)

        def x_flux(x, s):
            rows = [[Q[f, x + k, inner, :] for f in range(fields)] for k in range(1, 5)]
            s_next = speed_of(rows[2], 1)
            return interface_flux(*rows, jnp.maximum(s, s_next), 1), s_next

        def step(x, carry):
            before, s = carry
            after, s_next = x_flux(x, s)
            cells = [[Q[f, x + 2, PAD + k : PAD + k + cy, :] for f in range(fields)] for k in (-1, 0, 1, 2)]
            sy = jnp.abs(cells[1][2]) * RC[0, x] + RC[1, x]
            sy_next = jnp.where(row == cy - 1, SN[pl.ds(x, 1), :], pltpu.roll(sy, cy - 1, 0))
            flux = interface_flux(*cells, jnp.maximum(sy, sy_next), 2)
            outer = (lane < 2) | (lane >= cz - 2)
            for f in range(fields):
                low = jnp.where(row == 0, FL[f, pl.ds(x, 1), :], pltpu.roll(flux[f], 1, 0))
                along_z = jnp.where(outer, pltpu.roll(C[f], cz - 4 - 8 * x, 1), T[f, x])
                total = (after[f] - before[f]) + (flux[f] - low) + along_z
                update(f, x, cells[1][f], total)
            return tuple(after), s_next

        s = speed_of([Q[f, 1, inner, :] for f in range(fields)], 1)
        start, s = x_flux(-1, s)
        lax.fori_loop(0, cx, step, (tuple(start), s))

    load_state.wait()
    pack_y(Q1, Sy1, fields)
    pack_z(Q1, Pz.at[0], fields)
    mass = lax.fori_loop(
        0, cx, lambda x, m: m + Q1[0, x + 2, inner, :], jnp.zeros((cy, cz), jnp.float32)
    )
    M[0] = mass[:8] + mass[8:] if cy == 16 else jnp.broadcast_to(jnp.sum(mass, 0, keepdims=True) / 8, (8, cz))
    pl.semaphore_wait(barrier, gx + gy + gz - 3)
    x1, y1, z1 = exchange(Q1, Sy1, Ry1, Pz.at[0], Rz.at[0])
    masses = [send(M.at[0], Mx.at[k - 1], peer(0, k)) for k in range(1, gx)]

    load_phi.wait()
    boxes = cx // half
    here = me[0]

    def owned(slots_ref, owner, holder, j):
        slot = codes[0, 0, holder * boxes + j] - owner * slots
        mine = (slot >= 0) & (slot < slots)
        return jnp.where(mine, slots_ref[jnp.clip(slot, 0, slots - 1)], 0.0)

    steps = [d for k in range(1, gx - 1) for d in (k, -k)]
    direct = {d: channel() for d in steps}
    hand = [channel(), channel()]
    second, last = 1, gx - 2
    send_if(hand[0], here == 0, PH, Pf.at[0], {"gx": second})
    send_if(hand[1], here == gx - 1, PH, Pf.at[1], {"gx": last})
    for p in range(gx):
        for j in range(boxes):
            Ps[p, j] = owned(PH, here, p, j)
    inside = (here >= 1) & (here <= gx - 2)
    for d in steps:
        p = here + d
        now = inside & (p >= 0) & (p < gx) & ~((here == second) & (p > second)) & ~((here == last) & (p < last))
        at = jnp.clip(p, 0, gx - 1)
        send_if(direct[d], now, Ps.at[at], Pr.at[steps.index(d)], {"gx": at})

    def pass_on():
        for i, (via, owner) in enumerate(((second, 0), (last, gx - 1))):
            cond = here == via
            wait_if(hand[i], cond, Pf.at[i])
            targets = range(gx - 1, via, -1) if i == 0 else range(via)
            for p in targets:

                @pl.when(cond)
                def _():
                    for j in range(boxes):
                        Ps[p, j] = Ps[p, j] + owned(Pf.at[i], owner, p, j)

                send_if(direct[p - via], cond, Ps.at[p], Pr.at[steps.index(p - via)], {"gx": p})

    z_main(Q1)

    for copy in x1 + y1 + z1:
        copy.wait_recv()

    def to_first(f, x, q, total):
        Q2[f, x + 2, inner, :] = q - DTH * total

    finish(Q1, Sy1, Ry1, Pz.at[0], Rz.at[0], to_first)
    pack_y(Q2, Sy2, fields)
    pack_z(Q2, Pz.at[1], fields)
    x2, y2, z2 = exchange(Q2, Sy2, Ry2, Pz.at[1], Rz.at[1])

    for copy in masses:
        copy.wait_recv()
    M[1] = M[0] + sum(Mx[k] for k in range(gx - 1))
    masses = [send(M.at[1], My.at[k - 1], peer(1, k)) for k in range(1, gy)]

    pass_on()
    z_main(Q2)

    for copy in masses:
        copy.wait_recv()
    M[2] = M[1] + sum(My[k] for k in range(gy - 1))
    masses = [send(M.at[2], Mz.at[k - 1], peer(2, k)) for k in range(1, gz)]

    for copy in x2 + y2 + z2:
        copy.wait_recv()

    def to_new(f, x, q, total):
        value = 0.5 * Q1[f, x + 2, inner, :] + 0.5 * (q - DTH * total)
        NS[f, x] = value
        if f == 0:
            Dg[me[0] * boxes + x // half, x % half] = value

    block = lambda i: Dg.at[pl.ds(i * boxes, boxes)]
    spread = {d: channel() for k in range(1, gx) for d in (k, -k)}

    def send_density():
        for d in sorted(spread, key=lambda d: -abs(d)):
            if abs(d) < 3:
                to = here + d
                send_if(spread[d], (to >= 0) & (to < gx), block(here), block(here), {"gx": to})

    def relay_density():
        for d in sorted(spread, key=abs):
            if abs(d) >= 3:
                one = 1 if d > 0 else -1
                source, to = here - (d - one), here + one
                cond = (source >= 0) & (source < gx) & (to >= 0) & (to < gx)
                wait_if(spread[d - one], cond, block(source))
                send_if(spread[d], cond, block(source), block(source), {"gx": to})

    def wait_density():
        for d in spread:
            source, beyond = here - d, here + (1 if d > 0 else -1)
            relayed = (abs(d) >= 2) & (beyond >= 0) & (beyond < gx)
            wait_if(spread[d], (source >= 0) & (source < gx) & ~relayed, block(source))

    finish(Q2, Sy2, Ry2, Pz.at[1], Rz.at[1], to_new)
    send_density()
    out_state = pltpu.make_async_copy(NS, new_state, local_sem.at[2])
    out_state.start()
    for j in range(boxes):
        Qp[0, 2 + j * half : 2 + (j + 1) * half, inner, :] = owned(PH, here, here, j)

    def add_potential(cond, get):
        @pl.when(cond)
        def _():
            for j in range(boxes):
                at = slice(2 + j * half, 2 + (j + 1) * half)
                Qp[0, at, inner, :] = Qp[0, at, inner, :] + get(j)

    add_potential(here == second, lambda j: owned(Pf.at[0], 0, here, j))
    add_potential(here == last, lambda j: owned(Pf.at[1], gx - 1, here, j))
    for d in steps:
        source = here - d
        cond = (source >= 1) & (source <= gx - 2) & (here >= 0)
        wait_if(direct[d], cond, Pr.at[steps.index(d)])
        add_potential(cond, lambda j: Pr[steps.index(d), j])
    pack_y(Qp, Syp, 1)
    pack_z(Qp, Pzp, 1)
    xp, yp, zp = exchange(Qp, Syp, Ryp, Pzp, Rzp_)
    relay_density()

    for copy in masses:
        copy.wait_recv()
    total = M[2] + sum(Mz[k] for k in range(gz - 1))
    mean = jnp.sum(total) * (1.0 / (cx * cy * cz * gx * gy * gz))
    for copy in xp + yp + zp:
        copy.wait_recv()
    unpack_y(Qp, Ryp, 1)
    prev, nxt = from_both(Rzp_)
    beside = lambda v: pltpu.roll(v, 1, 1) + pltpu.roll(v, cz - 1, 1)
    Cp[...] = jnp.where(
        low_half, beside(jnp.where(low_half, Pzp[0], nxt[0])), beside(jnp.where(low_half, prev[0], Pzp[0]))
    )

    def poisson(x, carry):
        q = Qp[0, x + 2, inner, :]
        along_z = jnp.where((lane == 0) | (lane == cz - 1), pltpu.roll(Cp[...], cz - 4 - 8 * x, 1), beside(q))
        near = Qp[0, x + 1, inner, :] + Qp[0, x + 3, inner, :]
        near = near + Qp[0, x + 2, PAD - 1 : PAD - 1 + cy, :] + Qp[0, x + 2, PAD + 1 : PAD + 1 + cy, :]
        RS[x] = FOURPIG * (NS[0, x] - mean) - (near + along_z - 6.0 * q)
        return carry

    lax.fori_loop(0, cx, poisson, 0)
    out_residual = pltpu.make_async_copy(RS, residual, local_sem.at[3])
    out_residual.start()

    wait_density()
    for s in range(slots):
        wanted = me[0] * slots + s
        at = jnp.int32(-1)
        for b in range(gx * boxes):
            at = jnp.where(codes[0, 0, b] == wanted, b, at)
        DS[s] = jnp.where(at >= 0, Dg[jnp.maximum(at, 0)], 0.0)
    out_density = pltpu.make_async_copy(DS, density_solver, local_sem.at[4])
    out_density.start()
    for copy in sends:
        copy.wait_send()
    for cond, i, src in some_sends:
        pl.when(cond)(lambda: copy_on(i, src, src, peer(0, 1)).wait_send())
    out_state.wait()
    out_residual.wait()
    out_density.wait()


def on_device(sizes, state, solver_owner, phi_prev):
    fields, cx, cy, cz = state.shape
    slots, half = phi_prev.shape[:2]
    gx, gy, gz = sizes
    boxes = cx // half
    f32 = lambda *s: pltpu.VMEM(s, jnp.float32)
    padded = (cx + 4, cy + 2 * PAD, cz)
    n_send = 3 * (4 + min(gz - 1, 2)) + (gx + gy + gz - 3) + (2 * gx - 4) + 2 + (2 * gx - 2)
    out = lambda *s: jax.ShapeDtypeStruct(s, jnp.float32)
    hbm = pl.BlockSpec(memory_space=pl.ANY)
    return pl.pallas_call(
        functools.partial(kernel, (sizes, fields, cx, cy, cz, slots, half)),
        out_shape=(out(*state.shape), out(*phi_prev.shape), out(cx, cy, cz)),
        in_specs=[pl.BlockSpec(memory_space=pltpu.SMEM), hbm, hbm],
        out_specs=(hbm, hbm, hbm),
        scratch_shapes=[
            f32(fields, *padded), f32(fields, *padded), f32(1, *padded),
            f32(fields, 4, cx, cz), f32(fields, 4, cx, cz), f32(1, 4, cx, cz),
            f32(fields, 4, cx, cz), f32(fields, 4, cx, cz), f32(1, 4, cx, cz),
            f32(2, fields, cy, cz), f32(1, cy, cz), f32(2, 2, fields, cy, cz), f32(2, 1, cy, cz),
            f32(fields, cx, cy, cz), f32(2, cx, cy, cz), f32(fields, cx, cz), f32(cx, cz),
            f32(fields, cy, cz), f32(cy, cz),
            f32(slots, half, cy, cz), f32(gx, boxes, half, cy, cz), f32(2 * gx - 4, boxes, half, cy, cz), f32(2, slots, half, cy, cz),
            f32(fields, cx, cy, cz), f32(gx * boxes, half, cy, cz), f32(slots, half, cy, cz), f32(cx, cy, cz),
            f32(3, 8, cz), f32(gx - 1, 8, cz), f32(gy - 1, 8, cz), f32(gz - 1, 8, cz),
            pltpu.SemaphoreType.DMA((n_send,)), pltpu.SemaphoreType.DMA((n_send,)), pltpu.SemaphoreType.DMA((5,)),
        ],
        compiler_params=pltpu.CompilerParams(
            collective_id=0, has_side_effects=True, vmem_limit_bytes=63 * 1024 * 1024
        ),
    )(solver_owner, state, phi_prev)


def solution(mesh):
    sizes = tuple(mesh.shape[a] for a in AXES)
    placed = (P(None, "gx", "gy", "gz"), P("gy", "gz", None), P("gx", None, "gy", "gz"))
    return jax.shard_map(
        functools.partial(on_device, sizes),
        mesh=mesh,
        in_specs=placed,
        out_specs=(P(None, "gx", "gy", "gz"), P("gx", None, "gy", "gz"), P("gx", "gy", "gz")),
        check_vma=False,
    )
```

```python
import functools

import jax
import jax.numpy as jnp
from jax import lax
from jax.experimental import pallas as pl
from jax.experimental.pallas import tpu as pltpu
from jax.sharding import PartitionSpec as P

GAMMA = 5.0 / 3.0
DTH = 0.04
FOURPIG = 2.0
PAD = 8
AXES = ("gx", "gy", "gz")


def edge_value(a, b, c, d):
    e = 7.0 / 12.0 * (b + c) - 1.0 / 12.0 * (a + d)
    return jnp.minimum(jnp.maximum(e, jnp.minimum(b, c)), jnp.maximum(b, c))


def sound(q0, q5):
    rinv = 1.0 / jnp.maximum(q0, 0.25)
    return rinv, jnp.sqrt((GAMMA * (GAMMA - 1.0)) * jnp.maximum(q5, 0.1) * rinv)


def speed_of(q, d):
    rinv, c = sound(q[0], q[5])
    return jnp.abs(q[d]) * rinv + c


def interface_flux(a, b, c, d, far, direction):
    n = len(b)
    e = [edge_value(a[f], b[f], c[f], d[f]) for f in range(n)]
    vel = e[direction] / jnp.maximum(e[0], 0.25)
    press = (GAMMA - 1.0) * jnp.maximum(e[5], 0.1)
    half = 0.5 * far
    out = [e[direction]]
    for k in (1, 2, 3):
        term = e[k] * vel
        out.append(term + press if k == direction else term)
    out.append((e[4] + press) * vel)
    for k in range(5, n):
        out.append(e[k] * vel)
    return [out[f] - half * (c[f] - b[f]) for f in range(n)]


def lanes_change(q, s):
    n = q[0].shape[1]
    low = [pltpu.roll(v, 1, 1) for v in q]
    high = [pltpu.roll(v, n - 1, 1) for v in q]
    higher = [pltpu.roll(v, n - 2, 1) for v in q]
    flux = interface_flux(low, q, high, higher, jnp.maximum(s, pltpu.roll(s, n - 1, 1)), 3)
    return [v - pltpu.roll(v, 1, 1) for v in flux]


def kernel(
    shape, codes, state, phi, NS, DS, RS,
    Q1, Q2, Qp, Sy1, Sy2, Syp, Ry1, Ry2, Ryp, Pz, Pzp, Rz, Rzp_, T, RC, FL, SN, C, Cp,
    PH, Ps, Pr, Pf, Dg, M, Mx, My, Mz, send_sem, recv_sem, local_sem,
):
    sizes, fields, cx, cy, cz, slots, half = shape
    gx, gy, gz = sizes
    me = [lax.axis_index(a) for a in AXES]
    peer = lambda i, k: {AXES[i]: lax.rem(me[i] + k, sizes[i])}
    used = [0]
    sends = []

    def send(src, dst, to):
        i = used[0]
        used[0] += 1
        copy = pltpu.make_async_remote_copy(
            src_ref=src, dst_ref=dst, send_sem=send_sem.at[i], recv_sem=recv_sem.at[i],
            device_id=to, device_id_type=pl.DeviceIdType.MESH,
        )
        copy.start()
        sends.append(copy)
        return copy

    def channel():
        used[0] += 1
        return used[0] - 1

    def copy_on(i, src, dst, to):
        return pltpu.make_async_remote_copy(
            src_ref=src, dst_ref=dst, send_sem=send_sem.at[i], recv_sem=recv_sem.at[i],
            device_id=to, device_id_type=pl.DeviceIdType.MESH,
        )

    some_sends = []

    def send_if(i, cond, src, dst, to):
        pl.when(cond)(lambda: copy_on(i, src, dst, to).start())
        some_sends.append((cond, i, src))

    def wait_if(i, cond, dst):
        pl.when(cond)(lambda: copy_on(i, dst, dst, peer(0, 1)).wait_recv())

    load_state = pltpu.make_async_copy(
        state, Q1.at[:, pl.ds(2, cx), pl.ds(PAD, cy)], local_sem.at[0]
    )
    load_state.start()
    load_phi = pltpu.make_async_copy(phi, PH, local_sem.at[1])
    load_phi.start()

    barrier = pltpu.get_barrier_semaphore()
    for i in range(3):
        for k in range(1, sizes[i]):
            pl.semaphore_signal(
                barrier, inc=1, device_id=peer(i, k), device_id_type=pl.DeviceIdType.MESH
            )

    lane = lax.broadcasted_iota(jnp.int32, (cy, cz), 1)
    row = lax.broadcasted_iota(jnp.int32, (cy, cz), 0)
    group = lane // 8
    low_half = lane % 8 < 4
    inner = slice(PAD, PAD + cy)

    def pack_y(Q, Sy, n):
        flat = Q.reshape(n * (cx + 4) * (cy + 2 * PAD), cz)
        for f in range(n):
            for r, y in enumerate((0, 1, cy - 2, cy - 1)):
                at = (f * (cx + 4) + 2) * (cy + 2 * PAD) + PAD + y
                Sy[f, r] = flat[pl.ds(at, cx, stride=cy + 2 * PAD), :]

    def unpack_y(Q, Ry, n):
        flat = Q.reshape(n * (cx + 4) * (cy + 2 * PAD), cz)
        for f in range(n):
            for r, y in enumerate((-2, -1, cy, cy + 1)):
                at = (f * (cx + 4) + 2) * (cy + 2 * PAD) + PAD + y
                flat[pl.ds(at, cx, stride=cy + 2 * PAD), :] = Ry[f, r]

    def pack_z(Q, Pz, n):
        def step(x, packed):
            return tuple(
                jnp.where(group == x, pltpu.roll(Q[f, x + 2, inner, :], 4 + 8 * x, 1), packed[f])
                for f in range(n)
            )

        packed = lax.fori_loop(0, cx, step, tuple(jnp.zeros((cy, cz), jnp.float32) for _ in range(n)))
        for f in range(n):
            Pz[f] = packed[f]

    def exchange(Q, Sy, Ry, Pz, Rz):
        x = [
            send(Q.at[:, pl.ds(cx, 2), pl.ds(PAD, cy)], Q.at[:, pl.ds(0, 2), pl.ds(PAD, cy)], peer(0, 1)),
            send(Q.at[:, pl.ds(2, 2), pl.ds(PAD, cy)], Q.at[:, pl.ds(cx + 2, 2), pl.ds(PAD, cy)], peer(0, gx - 1)),
        ]
        y = [
            send(Sy.at[:, pl.ds(2, 2)], Ry.at[:, pl.ds(0, 2)], peer(1, 1)),
            send(Sy.at[:, pl.ds(0, 2)], Ry.at[:, pl.ds(2, 2)], peer(1, gy - 1)),
        ]
        z = [send(Pz, Rz.at[0], peer(2, 1))]
        if gz > 2:
            z.append(send(Pz, Rz.at[1], peer(2, gz - 1)))
        return x, y, z

    def from_both(Rz):
        return Rz.at[0], Rz.at[1 if gz > 2 else 0]

    def z_main(Q):
        def step(x, carry):
            q = [Q[f, x + 2, inner, :] for f in range(fields)]
            rinv, c = sound(q[0], q[5])
            RC[0, x] = rinv
            RC[1, x] = c
            change = lanes_change(q, jnp.abs(q[3]) * rinv + c)
            for f in range(fields):
                T[f, x] = change[f]
            return carry

        lax.fori_loop(0, cx, step, 0, unroll=2)

    def finish(Q, Sy, Ry, Pz, Rz, update):
        prev, nxt = from_both(Rz)
        left = [jnp.where(low_half, prev[f], Pz[f]) for f in range(fields)]
        left = lanes_change(left, speed_of(left, 3))
        right = [jnp.where(low_half, Pz[f], nxt[f]) for f in range(fields)]
        right = lanes_change(right, speed_of(right, 3))
        for f in range(fields):
            C[f] = jnp.where(low_half, right[f], left[f])
        unpack_y(Q, Ry, fields)
        b = [Ry[f, 1] for f in range(fields)]
        c = [Sy[f, 0] for f in range(fields)]
        flux = interface_flux(
            [Ry[f, 0] for f in range(fields)], b, c, [Sy[f, 1] for f in range(fields)],
            jnp.maximum(speed_of(b, 2), speed_of(c, 2)), 2,
        )
        for f in range(fields):
            FL[f] = flux[f]
        SN[...] = speed_of([Ry[f, 2] for f in range(fields)], 2)

        def x_flux(x, s):
            rows = [[Q[f, x + k, inner, :] for f in range(fields)] for k in range(1, 5)]
            s_next = speed_of(rows[2], 1)
            return interface_flux(*rows, jnp.maximum(s, s_next), 1), s_next

        def step(x, carry):
            before, s = carry
            after, s_next = x_flux(x, s)
            cells = [[Q[f, x + 2, PAD + k : PAD + k + cy, :] for f in range(fields)] for k in (-1, 0, 1, 2)]
            sy = jnp.abs(cells[1][2]) * RC[0, x] + RC[1, x]
            sy_next = jnp.where(row == cy - 1, SN[pl.ds(x, 1), :], pltpu.roll(sy, cy - 1, 0))
            flux = interface_flux(*cells, jnp.maximum(sy, sy_next), 2)
            outer = (lane < 2) | (lane >= cz - 2)
            for f in range(fields):
                low = jnp.where(row == 0, FL[f, pl.ds(x, 1), :], pltpu.roll(flux[f], 1, 0))
                along_z = jnp.where(outer, pltpu.roll(C[f], cz - 4 - 8 * x, 1), T[f, x])
                total = (after[f] - before[f]) + (flux[f] - low) + along_z
                update(f, x, cells[1][f], total)
            return tuple(after), s_next

        s = speed_of([Q[f, 1, inner, :] for f in range(fields)], 1)
        start, s = x_flux(-1, s)
        lax.fori_loop(0, cx, step, (tuple(start), s))

    load_state.wait()
    pack_y(Q1, Sy1, fields)
    pack_z(Q1, Pz.at[0], fields)
    mass = lax.fori_loop(
        0, cx, lambda x, m: m + Q1[0, x + 2, inner, :], jnp.zeros((cy, cz), jnp.float32)
    )
    M[0] = mass[:8] + mass[8:] if cy == 16 else jnp.broadcast_to(jnp.sum(mass, 0, keepdims=True) / 8, (8, cz))
    pl.semaphore_wait(barrier, gx + gy + gz - 3)
    x1, y1, z1 = exchange(Q1, Sy1, Ry1, Pz.at[0], Rz.at[0])
    masses = [send(M.at[0], Mx.at[k - 1], peer(0, k)) for k in range(1, gx)]

    load_phi.wait()
    boxes = cx // half
    here = me[0]

    def owned(slots_ref, owner, holder, j):
        slot = codes[0, 0, holder * boxes + j] - owner * slots
        mine = (slot >= 0) & (slot < slots)
        return jnp.where(mine, slots_ref[jnp.clip(slot, 0, slots - 1)], 0.0)

    steps = [d for k in range(1, gx - 1) for d in (k, -k)]
    direct = {d: channel() for d in steps}
    hand = [channel(), channel()]
    second, last = 1, gx - 2
    send_if(hand[0], here == 0, PH, Pf.at[0], {"gx": second})
    send_if(hand[1], here == gx - 1, PH, Pf.at[1], {"gx": last})
    for p in range(gx):
        for j in range(boxes):
            Ps[p, j] = owned(PH, here, p, j)
    inside = (here >= 1) & (here <= gx - 2)
    for d in steps:
        p = here + d
        now = inside & (p >= 0) & (p < gx) & ~((here == second) & (p > second)) & ~((here == last) & (p < last))
        at = jnp.clip(p, 0, gx - 1)
        send_if(direct[d], now, Ps.at[at], Pr.at[steps.index(d)], {"gx": at})

    def pass_on():
        for i, (via, owner) in enumerate(((second, 0), (last, gx - 1))):
            cond = here == via
            wait_if(hand[i], cond, Pf.at[i])
            targets = range(gx - 1, via, -1) if i == 0 else range(via)
            for p in targets:

                @pl.when(cond)
                def _():
                    for j in range(boxes):
                        Ps[p, j] = Ps[p, j] + owned(Pf.at[i], owner, p, j)

                send_if(direct[p - via], cond, Ps.at[p], Pr.at[steps.index(p - via)], {"gx": p})

    z_main(Q1)

    for copy in x1 + y1 + z1:
        copy.wait_recv()

    def to_first(f, x, q, total):
        Q2[f, x + 2, inner, :] = q - DTH * total

    finish(Q1, Sy1, Ry1, Pz.at[0], Rz.at[0], to_first)
    pack_y(Q2, Sy2, fields)
    pack_z(Q2, Pz.at[1], fields)
    x2, y2, z2 = exchange(Q2, Sy2, Ry2, Pz.at[1], Rz.at[1])

    for copy in masses:
        copy.wait_recv()
    M[1] = M[0] + sum(Mx[k] for k in range(gx - 1))
    masses = [send(M.at[1], My.at[k - 1], peer(1, k)) for k in range(1, gy)]

    pass_on()
    z_main(Q2)

    for copy in masses:
        copy.wait_recv()
    M[2] = M[1] + sum(My[k] for k in range(gy - 1))
    masses = [send(M.at[2], Mz.at[k - 1], peer(2, k)) for k in range(1, gz)]

    for copy in x2 + y2 + z2:
        copy.wait_recv()

    def to_new(f, x, q, total):
        value = 0.5 * Q1[f, x + 2, inner, :] + 0.5 * (q - DTH * total)
        NS[f, x] = value
        if f == 0:
            Dg[me[0] * boxes + x // half, x % half] = value

    block = lambda i: Dg.at[pl.ds(i * boxes, boxes)]
    spread = {d: channel() for k in range(1, gx) for d in (k, -k)}

    def send_density():
        for d in sorted(spread, key=lambda d: -abs(d)):
            if abs(d) < 3:
                to = here + d
                send_if(spread[d], (to >= 0) & (to < gx), block(here), block(here), {"gx": to})

    def relay_density():
        for d in sorted(spread, key=abs):
            if abs(d) >= 3:
                one = 1 if d > 0 else -1
                source, to = here - (d - one), here + one
                cond = (source >= 0) & (source < gx) & (to >= 0) & (to < gx)
                wait_if(spread[d - one], cond, block(source))
                send_if(spread[d], cond, block(source), block(source), {"gx": to})

    def wait_density():
        for d in spread:
            source, beyond = here - d, here + (1 if d > 0 else -1)
            relayed = (abs(d) >= 2) & (beyond >= 0) & (beyond < gx)
            wait_if(spread[d], (source >= 0) & (source < gx) & ~relayed, block(source))

    finish(Q2, Sy2, Ry2, Pz.at[1], Rz.at[1], to_new)
    send_density()
    for j in range(boxes):
        Qp[0, 2 + j * half : 2 + (j + 1) * half, inner, :] = owned(PH, here, here, j)

    def add_potential(cond, get):
        @pl.when(cond)
        def _():
            for j in range(boxes):
                at = slice(2 + j * half, 2 + (j + 1) * half)
                Qp[0, at, inner, :] = Qp[0, at, inner, :] + get(j)

    add_potential(here == second, lambda j: owned(Pf.at[0], 0, here, j))
    add_potential(here == last, lambda j: owned(Pf.at[1], gx - 1, here, j))
    for d in steps:
        source = here - d
        cond = (source >= 1) & (source <= gx - 2) & (here >= 0)
        wait_if(direct[d], cond, Pr.at[steps.index(d)])
        add_potential(cond, lambda j: Pr[steps.index(d), j])
    pack_y(Qp, Syp, 1)
    pack_z(Qp, Pzp, 1)
    xp, yp, zp = exchange(Qp, Syp, Ryp, Pzp, Rzp_)
    relay_density()

    for copy in masses:
        copy.wait_recv()
    total = M[2] + sum(Mz[k] for k in range(gz - 1))
    mean = jnp.sum(total) * (1.0 / (cx * cy * cz * gx * gy * gz))
    for copy in xp + yp + zp:
        copy.wait_recv()
    unpack_y(Qp, Ryp, 1)
    prev, nxt = from_both(Rzp_)
    beside = lambda v: pltpu.roll(v, 1, 1) + pltpu.roll(v, cz - 1, 1)
    Cp[...] = jnp.where(
        low_half, beside(jnp.where(low_half, Pzp[0], nxt[0])), beside(jnp.where(low_half, prev[0], Pzp[0]))
    )

    def poisson(x, carry):
        q = Qp[0, x + 2, inner, :]
        along_z = jnp.where((lane == 0) | (lane == cz - 1), pltpu.roll(Cp[...], cz - 4 - 8 * x, 1), beside(q))
        near = Qp[0, x + 1, inner, :] + Qp[0, x + 3, inner, :]
        near = near + Qp[0, x + 2, PAD - 1 : PAD - 1 + cy, :] + Qp[0, x + 2, PAD + 1 : PAD + 1 + cy, :]
        RS[x] = FOURPIG * (NS[0, x] - mean) - (near + along_z - 6.0 * q)
        return carry

    lax.fori_loop(0, cx, poisson, 0)

    wait_density()
    for s in range(slots):
        wanted = me[0] * slots + s
        at = jnp.int32(-1)
        for b in range(gx * boxes):
            at = jnp.where(codes[0, 0, b] == wanted, b, at)
        DS[s] = jnp.where(at >= 0, Dg[jnp.maximum(at, 0)], 0.0)
    for copy in sends:
        copy.wait_send()
    for cond, i, src in some_sends:
        pl.when(cond)(lambda: copy_on(i, src, src, peer(0, 1)).wait_send())


def write_out(*refs):
    n = len(refs) // 2
    sem = refs[-1]
    copies = [pltpu.make_async_copy(refs[i], refs[n + i], sem.at[i]) for i in range(n)]
    for copy in copies:
        copy.start()
    for copy in copies:
        copy.wait()


def on_device(sizes, state, solver_owner, phi_prev):
    fields, cx, cy, cz = state.shape
    slots, half = phi_prev.shape[:2]
    gx, gy, gz = sizes
    boxes = cx // half
    f32 = lambda *s: pltpu.VMEM(s, jnp.float32)
    padded = (cx + 4, cy + 2 * PAD, cz)
    n_send = 3 * (4 + min(gz - 1, 2)) + (gx + gy + gz - 3) + (2 * gx - 4) + 2 + (2 * gx - 2)
    out = lambda *s: jax.ShapeDtypeStruct(s, jnp.float32)
    hbm = pl.BlockSpec(memory_space=pl.ANY)
    vmem = pl.BlockSpec(memory_space=pltpu.VMEM)
    results = pl.pallas_call(
        functools.partial(kernel, (sizes, fields, cx, cy, cz, slots, half)),
        out_shape=(out(*state.shape), out(*phi_prev.shape), out(cx, cy, cz)),
        in_specs=[pl.BlockSpec(memory_space=pltpu.SMEM)] + [pl.BlockSpec(memory_space=pltpu.HBM)] * 2,
        out_specs=(vmem, vmem, vmem),
        scratch_shapes=[
            f32(fields, *padded), f32(fields, *padded), f32(1, *padded),
            f32(fields, 4, cx, cz), f32(fields, 4, cx, cz), f32(1, 4, cx, cz),
            f32(fields, 4, cx, cz), f32(fields, 4, cx, cz), f32(1, 4, cx, cz),
            f32(2, fields, cy, cz), f32(1, cy, cz), f32(2, 2, fields, cy, cz), f32(2, 1, cy, cz),
            f32(fields, cx, cy, cz), f32(2, cx, cy, cz), f32(fields, cx, cz), f32(cx, cz),
            f32(fields, cy, cz), f32(cy, cz),
            f32(slots, half, cy, cz), f32(gx, boxes, half, cy, cz), f32(2 * gx - 4, boxes, half, cy, cz), f32(2, slots, half, cy, cz),
            f32(gx * boxes, half, cy, cz),
            f32(3, 8, cz), f32(gx - 1, 8, cz), f32(gy - 1, 8, cz), f32(gz - 1, 8, cz),
            pltpu.SemaphoreType.DMA((n_send,)), pltpu.SemaphoreType.DMA((n_send,)), pltpu.SemaphoreType.DMA((2,)),
        ],
        compiler_params=pltpu.CompilerParams(
            collective_id=0, has_side_effects=True, vmem_limit_bytes=48 * 1024 * 1024
        ),
    )(solver_owner, state, phi_prev)
    return pl.pallas_call(
        write_out,
        out_shape=tuple(out(*r.shape) for r in results),
        in_specs=[hbm] * 3,
        out_specs=(pl.BlockSpec(memory_space=pltpu.HBM),) * 3,
        scratch_shapes=[pltpu.SemaphoreType.DMA((3,))],
        compiler_params=pltpu.CompilerParams(vmem_limit_bytes=16 * 1024 * 1024),
    )(*results)


def solution(mesh):
    sizes = tuple(mesh.shape[a] for a in AXES)
    placed = (P(None, "gx", "gy", "gz"), P("gy", "gz", None), P("gx", None, "gy", "gz"))
    return jax.shard_map(
        functools.partial(on_device, sizes),
        mesh=mesh,
        in_specs=placed,
        out_specs=(P(None, "gx", "gy", "gz"), P("gx", None, "gy", "gz"), P("gx", "gy", "gz")),
        check_vma=False,
    )
```
